32 devices in a mesh: job: 2 (over core), replica: 4 (over z), model: 4 (over y, x).
Axes of the slice: x: 2, y: 2, z: 4, core: 2. Of those that a mesh axis runs over, the one named last changes fastest.
Arguments:
- grad_query: float32 [8, 1024, 1024], P(('job', 'replica'), None, 'model'), parts along dimension 0, may hold values from -0.875 to 0.875
- grad_key: float32 [8, 1024, 1024], P(('job', 'replica'), None, 'model'), parts along dimension 0, may hold values from -0.875 to 0.875
- grad_value: float32 [8, 1024, 1024], P(('job', 'replica'), None, 'model'), parts along dimension 0, may hold values from -0.875 to 0.875
- grad_mixed: float32 [8, 1024, 1024], P(('job', 'replica'), 'model'), parts along dimension 0, may hold values from -0.875 to 0.875
- grad_norm: float32 [8, 1024], P(('job', 'replica')), parts along dimension 0, may hold values from -8 to 8
- weight_query: float32 [2048, 1024], P(('job', 'replica'), 'model'), parts along dimension 0, may hold values from -0.25 to 0.25
- weight_key: float32 [2048, 1024], P(('job', 'replica'), 'model'), parts along dimension 0, may hold values from -0.25 to 0.25
- weight_value: float32 [2048, 1024], P(('job', 'replica'), 'model'), parts along dimension 0, may hold values from -0.25 to 0.25
- weight_mixed: float32 [2048, 1024], P(('job', 'model'), 'replica'), parts along dimension 0, may hold values from -0.25 to 0.25
- weight_norm: float32 [2048], P(('job', 'replica')), parts along dimension 0, may hold values from 0.25 to 1.75
- moment_query: float32 [2048, 1024], P(('job', 'replica'), 'model'), parts along dimension 0, may hold values from -0.1875 to 0.1875
- moment_key: float32 [2048, 1024], P(('job', 'replica'), 'model'), parts along dimension 0, may hold values from -0.1875 to 0.1875
- moment_value: float32 [2048, 1024], P(('job', 'replica'), 'model'), parts along dimension 0, may hold values from -0.1875 to 0.1875
- moment_mixed: float32 [2048, 1024], P(('job', 'model'), 'replica'), parts along dimension 0, may hold values from -0.1875 to 0.1875
- moment_norm: float32 [2048], P(('job', 'replica')), parts along dimension 0, may hold values from -1.75 to 1.75
Outputs:
- copy_query: bfloat16 [2048, 1024], P('job', 'model'), parts along dimension 0
- copy_key: bfloat16 [2048, 1024], P('job', 'model'), parts along dimension 0
- copy_value: bfloat16 [2048, 1024], P('job', 'model'), parts along dimension 0
- copy_mixed: bfloat16 [2048, 1024], P(('job', 'model')), parts along dimension 0
- copy_norm: bfloat16 [2048], P('job'), parts along dimension 0
- new_query: float32 [2048, 1024], P(('job', 'replica'), 'model'), parts along dimension 0
- new_key: float32 [2048, 1024], P(('job', 'replica'), 'model'), parts along dimension 0
- new_value: float32 [2048, 1024], P(('job', 'replica'), 'model'), parts along dimension 0
- new_mixed: float32 [2048, 1024], P(('job', 'model'), 'replica'), parts along dimension 0
- new_norm: float32 [2048], P(('job', 'replica')), parts along dimension 0
- state_new_query: float32 [2048, 1024], P(('job', 'replica'), 'model'), parts along dimension 0
- state_new_key: float32 [2048, 1024], P(('job', 'replica'), 'model'), parts along dimension 0
- state_new_value: float32 [2048, 1024], P(('job', 'replica'), 'model'), parts along dimension 0
- state_new_mixed: float32 [2048, 1024], P(('job', 'model'), 'replica'), parts along dimension 0
- state_new_norm: float32 [2048], P(('job', 'replica')), parts along dimension 0
The draws below stay inside these ranges and needn't reach their ends.
There are 2 independent parts, one for each index of `job`. The reference program is written for one: setup_inputs(seed, part) draws one part's arguments, and reference() takes and returns one part's arrays. A program takes and returns all parts, laid end to end along the dimension named above; each array names one. Nothing has to cross between parts.
All inputs are finite; a program needn't handle non-finite values.
Results may differ from the reference program's by a relative error of at most 0.0004.
Values may be sent and summed in bfloat16 or wider, within the bound.
A program may use at most 64 MiB of HBM per device.

```python
import jax
import jax.numpy as jnp
from jax import lax

WIDTH = 1024
ATTN = 1024
REPLICAS = 4


def with_spikes(result, stream_key, source, target, blocks, factor):
    def block_of(axis_at):
        return (jnp.arange(result.shape[axis_at]) // (result.shape[axis_at] // blocks)).reshape((-1,) + (1,) * (result.ndim - 1 - axis_at))

    near = jax.random.permutation(stream_key, blocks)[block_of(target)]
    other_side = (block_of(target) + blocks // 2) % blocks
    return jnp.where((block_of(source) == near) | (block_of(source) == other_side), factor * result, result)


def levels(rng, extent, shards, low, largest):
    loudness, own = 1.0, jax.random.fold_in(rng, 6)
    for axis_at, shards_of in shards:
        steps = jnp.exp(jax.random.uniform(jax.random.fold_in(own, axis_at), (shards_of,), jnp.float32, low / len(shards), largest / len(shards)))
        loudness = loudness * jnp.repeat(steps, extent[axis_at] // shards_of).reshape([-1 if axis == axis_at else 1 for axis in range(len(extent))])
    return loudness


def noise(rng, dims, width, bound, pieces=(), dtype=jnp.bfloat16):
    entries = jax.random.normal(rng, dims, jnp.float32) * width
    if len(pieces) > 0:
        entries = levels(rng, dims, pieces, -0.22, 0.18) * entries
    return jnp.clip(entries, min=-bound, max=bound).astype(dtype)


def heavy_noise(stream_key, dims, width, most, pieces, heavy, dtype=jnp.bfloat16):
    result = width * jax.random.normal(stream_key, dims, jnp.float32)
    if pieces:
        result = result * levels(stream_key, dims, pieces, -0.22, 0.18)
    return jnp.clip(with_spikes(result, jax.random.fold_in(stream_key, 3), *heavy), -most, most).astype(dtype)


def setup_inputs(seed: int = 0, part: int = 0) -> dict:
    streams_of = jax.random.split(jax.random.key(seed), 16)
    part_splits = jax.random.split(jax.random.fold_in(streams_of[15], part), 16)
    return {
        "grad_query": heavy_noise(part_splits[0], (REPLICAS, WIDTH, ATTN), 0.1, 0.875, ((0, 4), (2, 4)), (0, 1, 4, 2.0), jnp.float32),
        "grad_key": heavy_noise(part_splits[1], (REPLICAS, WIDTH, ATTN), 0.1, 0.875, ((0, 4), (2, 4)), (0, 1, 4, 2.0), jnp.float32),
        "grad_value": heavy_noise(part_splits[2], (REPLICAS, WIDTH, ATTN), 0.1, 0.875, ((0, 4), (2, 4)), (0, 1, 4, 2.0), jnp.float32),
        "grad_mixed": heavy_noise(part_splits[3], (REPLICAS, ATTN, WIDTH), 0.1, 0.875, ((0, 4), (1, 4)), (0, 2, 4, 2.0), jnp.float32),
        "grad_norm": heavy_noise(part_splits[4], (REPLICAS, WIDTH), 1.0, 8.0, ((0, 4),), (0, 1, 4, 2.0), jnp.float32),
        "weight_query": heavy_noise(part_splits[5], (WIDTH, ATTN), WIDTH ** -0.5, 0.25, ((0, 4), (1, 4)), (1, 0, 4, 2.0), jnp.float32),
        "weight_key": heavy_noise(part_splits[6], (WIDTH, ATTN), WIDTH ** -0.5, 0.25, ((0, 4), (1, 4)), (1, 0, 4, 2.0), jnp.float32),
        "weight_value": heavy_noise(part_splits[7], (WIDTH, ATTN), WIDTH ** -0.5, 0.25, ((0, 4), (1, 4)), (1, 0, 4, 2.0), jnp.float32),
        "weight_mixed": heavy_noise(part_splits[8], (ATTN, WIDTH), ATTN ** -0.5, 0.25, ((0, 4), (1, 4)), (0, 1, 4, 2.0), jnp.float32),
        "weight_norm": jnp.clip(1.0 + 0.15 * jax.random.normal(part_splits[9], (WIDTH,), jnp.float32), 0.25, 1.75),
        "moment_query": noise(part_splits[10], (WIDTH, ATTN), WIDTH ** -0.5, 0.1875, ((0, 4), (1, 4)), jnp.float32),
        "moment_key": noise(part_splits[11], (WIDTH, ATTN), WIDTH ** -0.5, 0.1875, ((0, 4), (1, 4)), jnp.float32),
        "moment_value": noise(part_splits[12], (WIDTH, ATTN), WIDTH ** -0.5, 0.1875, ((0, 4), (1, 4)), jnp.float32),
        "moment_mixed": noise(part_splits[13], (ATTN, WIDTH), ATTN ** -0.5, 0.1875, ((0, 4), (1, 4)), jnp.float32),
        "moment_norm": noise(part_splits[14], (WIDTH,), 0.3, 1.75, ((0, 4),), jnp.float32),
    }


learn_rate = 0.5
hold_rate = 0.9

def reference(grad_query, grad_key, grad_value, grad_mixed, grad_norm, weight_query, weight_key, weight_value, weight_mixed, weight_norm, moment_query, moment_key, moment_value, moment_mixed, moment_norm):
    mean_query = lax.optimization_barrier(jnp.sum(grad_query.astype(jnp.float32), axis=0)) * REPLICAS ** (-0.5)
    mean_key = lax.optimization_barrier(jnp.sum(grad_key.astype(jnp.float32), axis=0)) * REPLICAS ** (-0.5)
    mean_value = lax.optimization_barrier(jnp.sum(grad_value.astype(jnp.float32), axis=0)) * REPLICAS ** (-0.5)
    mean_mixed = lax.optimization_barrier(jnp.sum(grad_mixed.astype(jnp.float32), axis=0)) * REPLICAS ** (-0.5)
    mean_norm = lax.optimization_barrier(jnp.sum(grad_norm.astype(jnp.float32), axis=0)) * REPLICAS ** (-0.5)
    ratio_query = jnp.sqrt(lax.optimization_barrier(jnp.sum(weight_query * weight_query, axis=1, keepdims=True))) * lax.rsqrt(lax.optimization_barrier(jnp.sum(mean_query * mean_query, axis=1, keepdims=True)) + 1e-06)
    mean_query = mean_query * ratio_query
    ratio_key = jnp.sqrt(lax.optimization_barrier(jnp.sum(weight_key * weight_key, axis=1, keepdims=True))) * lax.rsqrt(lax.optimization_barrier(jnp.sum(mean_key * mean_key, axis=1, keepdims=True)) + 1e-06)
    mean_key = mean_key * ratio_key
    ratio_value = jnp.sqrt(lax.optimization_barrier(jnp.sum(weight_value * weight_value, axis=1, keepdims=True))) * lax.rsqrt(lax.optimization_barrier(jnp.sum(mean_value * mean_value, axis=1, keepdims=True)) + 1e-06)
    mean_value = mean_value * ratio_value
    ratio_mixed = jnp.sqrt(lax.optimization_barrier(jnp.sum(weight_mixed * weight_mixed, axis=0, keepdims=True))) * lax.rsqrt(lax.optimization_barrier(jnp.sum(mean_mixed * mean_mixed, axis=0, keepdims=True)) + 1e-06)
    mean_mixed = mean_mixed * ratio_mixed
    state_new_query = hold_rate * moment_query + mean_query
    new_query = weight_query - learn_rate * state_new_query
    state_new_key = hold_rate * moment_key + mean_key
    new_key = weight_key - learn_rate * state_new_key
    state_new_value = hold_rate * moment_value + mean_value
    new_value = weight_value - learn_rate * state_new_value
    state_new_mixed = hold_rate * moment_mixed + mean_mixed
    new_mixed = weight_mixed - learn_rate * state_new_mixed
    state_new_norm = hold_rate * moment_norm + mean_norm
    new_norm = weight_norm - learn_rate * state_new_norm
    copy_query = new_query.astype(jnp.bfloat16)
    copy_key = new_key.astype(jnp.bfloat16)
    copy_value = new_value.astype(jnp.bfloat16)
    copy_mixed = new_mixed.astype(jnp.bfloat16)
    copy_norm = new_norm.astype(jnp.bfloat16)
    return (copy_query, copy_key, copy_value, copy_mixed, copy_norm, new_query, new_key, new_value, new_mixed, new_norm, state_new_query, state_new_key, state_new_value, state_new_mixed, state_new_norm)
```

```python
import functools

import jax
import jax.numpy as jnp
from jax import lax
from jax.experimental import pallas as pl
from jax.experimental.pallas import tpu as pltpu
from jax.sharding import PartitionSpec as P

learn_rate = 0.5
hold_rate = 0.9


def local(
    grad_query,
    grad_key,
    grad_value,
    grad_mixed,
    grad_norm,
    weight_query,
    weight_key,
    weight_value,
    weight_mixed,
    weight_norm,
    moment_query,
    moment_key,
    moment_value,
    moment_mixed,
    moment_norm,
):
    mean_query, mean_key, mean_value, mean_mixed = (
        lax.psum_scatter(grad_query[0], "replica", scatter_dimension=0, tiled=True),
        lax.psum_scatter(grad_key[0], "replica", scatter_dimension=0, tiled=True),
        lax.psum_scatter(grad_value[0], "replica", scatter_dimension=0, tiled=True),
        lax.psum_scatter(grad_mixed[0], "replica", scatter_dimension=1, tiled=True),
    )
    whole_norm = lax.psum(grad_norm[0], "replica")
    place = lax.axis_index("replica")
    mean_norm = lax.dynamic_slice_in_dim(
        whole_norm, place * weight_norm.shape[0], weight_norm.shape[0]
    )
    mean_rate = lax.axis_size("replica") ** (-0.5)
    mean_query = mean_query * mean_rate
    mean_key = mean_key * mean_rate
    mean_value = mean_value * mean_rate
    mean_mixed = mean_mixed * mean_rate
    mean_norm = mean_norm * mean_rate
    (
        own_query,
        own_key,
        own_value,
        own_mixed,
        slope_query_norm,
        slope_key_norm,
        slope_value_norm,
        slope_mixed_norm,
    ) = lax.psum(
        (
            jnp.sum(weight_query * weight_query, axis=1, keepdims=True),
            jnp.sum(weight_key * weight_key, axis=1, keepdims=True),
            jnp.sum(weight_value * weight_value, axis=1, keepdims=True),
            jnp.sum(weight_mixed * weight_mixed, axis=0, keepdims=True),
            jnp.sum(mean_query * mean_query, axis=1, keepdims=True),
            jnp.sum(mean_key * mean_key, axis=1, keepdims=True),
            jnp.sum(mean_value * mean_value, axis=1, keepdims=True),
            jnp.sum(mean_mixed * mean_mixed, axis=0, keepdims=True),
        ),
        "model",
    )
    mean_query = mean_query * (jnp.sqrt(own_query) * lax.rsqrt(slope_query_norm + 1e-06))
    mean_key = mean_key * (jnp.sqrt(own_key) * lax.rsqrt(slope_key_norm + 1e-06))
    mean_value = mean_value * (jnp.sqrt(own_value) * lax.rsqrt(slope_value_norm + 1e-06))
    mean_mixed = mean_mixed * (jnp.sqrt(own_mixed) * lax.rsqrt(slope_mixed_norm + 1e-06))
    state_new_query = hold_rate * moment_query + mean_query
    new_query = weight_query - learn_rate * state_new_query
    state_new_key = hold_rate * moment_key + mean_key
    new_key = weight_key - learn_rate * state_new_key
    state_new_value = hold_rate * moment_value + mean_value
    new_value = weight_value - learn_rate * state_new_value
    state_new_mixed = hold_rate * moment_mixed + mean_mixed
    new_mixed = weight_mixed - learn_rate * state_new_mixed
    state_new_norm = hold_rate * moment_norm + mean_norm
    new_norm = weight_norm - learn_rate * state_new_norm
    copy_query, copy_key, copy_value, copy_mixed, copy_norm = (
        lax.all_gather(new_query.astype(jnp.bfloat16), "replica", axis=0, tiled=True),
        lax.all_gather(new_key.astype(jnp.bfloat16), "replica", axis=0, tiled=True),
        lax.all_gather(new_value.astype(jnp.bfloat16), "replica", axis=0, tiled=True),
        lax.all_gather(new_mixed.astype(jnp.bfloat16), "replica", axis=1, tiled=True),
        lax.all_gather(new_norm.astype(jnp.bfloat16), "replica", axis=0, tiled=True),
    )
    return (
        copy_query,
        copy_key,
        copy_value,
        copy_mixed,
        copy_norm,
        new_query,
        new_key,
        new_value,
        new_mixed,
        new_norm,
        state_new_query,
        state_new_key,
        state_new_value,
        state_new_mixed,
        state_new_norm,
    )


MESH = pl.DeviceIdType.MESH
EPS = 1e-06
SPAN = 228.0
FLOOR = 2.0 ** (-125 / 32)


def encode(x, scale):
    b = jnp.abs(x) * ((SPAN * FLOOR) / scale) + FLOOR
    for _ in range(5):
        b = b * b
    return jnp.where(x < 0.0, -b, b).astype(jnp.bfloat16)


def decode(y, scale):
    y = y.astype(jnp.float32)
    r = jnp.abs(y)
    for _ in range(4):
        r = lax.rsqrt(r)
    u = (r * lax.rsqrt(r) - FLOOR) * (scale * (1.0 / (SPAN * FLOOR)))
    return jnp.where(y < 0.0, -u, u)


def kernel(n, nm, mats, *refs):
    k = len(mats)
    refs = list(refs)

    def take(count):
        out = refs[:count]
        del refs[:count]
        return out

    grads, (gnorm_in,) = take(k), take(1)
    weights, (wnorm_in,) = take(k), take(1)
    moments, (mnorm_in,) = take(k), take(1)
    copies, (copy_norm,) = take(k), take(1)
    news, (new_norm,) = take(k), take(1)
    states, (state_norm,) = take(k), take(1)
    G, W, M, enc, got, total, stat, statg, ng, nw, nmo = take(11)
    gsem, wsem, msem, rs_s, rs_r, ag_s, ag_r, st_s, st_r, no_s, no_r = take(11)

    rows, cols = W.shape[1], W.shape[2]
    block = 64
    me = lax.axis_index("replica")
    mm = lax.axis_index("model")
    rate = n ** (-0.5)

    def part(ref, m, t):
        if mats[m] == 0:
            return ref.at[pl.ds(pl.multiple_of(t * rows, rows), rows), :]
        return ref.at[:, pl.ds(pl.multiple_of(t * cols, cols), cols)]

    def g_copy(m, t):
        return pltpu.make_async_copy(part(grads[m].at[0], m, t), G.at[m, t], gsem.at[m, t])

    def w_copy(m):
        return pltpu.make_async_copy(weights[m], W.at[m], wsem.at[m])

    def m_copy(m):
        return pltpu.make_async_copy(moments[m], M.at[m], msem.at[m])

    barrier = pltpu.get_barrier_semaphore()
    for d in range(1, n):
        pl.semaphore_signal(barrier, 1, device_id={"replica": lax.rem(me + d, n)}, device_id_type=MESH)
    for d in range(1, nm):
        pl.semaphore_signal(barrier, 1, device_id={"model": lax.rem(mm + d, nm)}, device_id_type=MESH)
    for m in range(k):
        for t in range(n):
            g_copy(m, t).start()
        w_copy(m).start()
        m_copy(m).start()

    near = jnp.where(2 * me < n, 0, 1)

    def mirror(direction, i):
        return jnp.where(direction == 0, i, n - 1 - i)

    def rs_copy(direction, m, t, to):
        return pltpu.make_async_remote_copy(
            src_ref=enc.at[direction, m, t], dst_ref=got.at[direction, m, t],
            send_sem=rs_s.at[direction, m, t], recv_sem=rs_r.at[direction, m, t],
            device_id={"replica": to}, device_id_type=MESH)

    def neighbour(direction):
        return jnp.clip(jnp.where(direction == 0, me + 1, me - 1), 0, n - 1)

    def blocks(body):
        @pl.loop(0, rows // block)
        def _(i):
            body(pl.ds(pl.multiple_of(i * block, block), block))

    def scale_of(direction, m, t):
        return got[direction, m, t, rows:rows + 8, :].astype(jnp.float32)[0:1]

    def rs_step(m, direction, s):
        place = mirror(direction, me)
        t = mirror(direction, n - 1 - s)

        @pl.when((n - 1 - s > place) & (place > 0))
        def _():
            rs_copy(direction, m, t, neighbour(direction)).wait_recv()
            scale = scale_of(direction, m, t)

            def body(r):
                G[m, t, r, :] = G[m, t, r, :] + decode(got[direction, m, t, r, :], scale)
            blocks(body)

        @pl.when(n - 1 - s > place)
        def _():
            def largest(i, top):
                x = jnp.abs(G[m, t, pl.ds(pl.multiple_of(i * block, block), block), :])
                return jnp.maximum(top, jnp.max(x.reshape(block // 8, 8, cols), axis=0))

            top = lax.fori_loop(0, rows // block, largest, jnp.zeros((8, cols), jnp.float32))
            top = jnp.max(top, axis=0, keepdims=True) * 1.0079 + 1e-30
            top = jnp.broadcast_to(top, (8, cols)).astype(jnp.bfloat16)
            enc[direction, m, t, rows:rows + 8, :] = top
            scale = top.astype(jnp.float32)[0:1]

            def body(r):
                enc[direction, m, t, r, :] = encode(G[m, t, r, :], scale)
            blocks(body)
            rs_copy(direction, m, t, neighbour(direction)).start()

    def stat_copy(m, d):
        peer = lax.rem(mm + d, nm)
        return pltpu.make_async_remote_copy(
            src_ref=stat.at[m], dst_ref=statg.at[m, d - 1], send_sem=st_s.at[m, d - 1], recv_sem=st_r.at[m, d - 1],
            device_id={"model": peer}, device_id_type=MESH)

    def squares(x, dim):
        x = x * x
        if dim == 1:
            return jnp.sum(x, axis=0, keepdims=True)
        half = functools.reduce(jnp.add, [x[:, c:c + 128] for c in range(0, cols, 128)])
        return jnp.sum(half.T, axis=0, keepdims=True)

    def own_stat(m):
        w_copy(m).wait()
        stat[m, 0:1, :] = squares(W[m], mats[m])

    def total_of(m):
        for direction in range(2):
            @pl.when(mirror(direction, me) > 0)
            def _():
                rs_copy(direction, m, me, neighbour(direction)).wait_recv()

        def add(*directions):
            scales = {d: scale_of(d, m, me) for d in directions}

            def body(r):
                u = functools.reduce(jnp.add, [decode(got[d, m, me, r, :], scales[d]) for d in directions])
                total[m, r, :] = (G[m, me, r, :] + u) * rate
            blocks(body)

        pl.when(me == 0)(lambda: add(1))
        pl.when(me == n - 1)(lambda: add(0))
        pl.when((me > 0) & (me < n - 1))(lambda: add(0, 1))
        stat[m, 1:2, :] = squares(total[m], mats[m])
        for d in range(1, nm):
            stat_copy(m, d).start()

    def ag_copy(direction, m, t):
        piece = part(copies[m], m, t)
        return pltpu.make_async_remote_copy(
            src_ref=piece, dst_ref=piece, send_sem=ag_s.at[direction, m, t], recv_sem=ag_r.at[direction, m, t],
            device_id={"replica": neighbour(direction)}, device_id_type=MESH)

    def update(m):
        for d in range(1, nm):
            stat_copy(m, d).wait_recv()
        sums = stat[m]
        for d in range(nm - 1):
            sums = sums + statg[m, d]
        ratio = jnp.sqrt(sums[0:1]) * lax.rsqrt(sums[1:2] + EPS)
        if mats[m] == 0:
            turned = jnp.broadcast_to(ratio, (128, rows)).T
            ratio = jnp.concatenate([turned] * (cols // 128), axis=1)
        m_copy(m).wait()
        state = hold_rate * M[m] + total[m] * ratio
        new = W[m] - learn_rate * state
        states[m][...] = state
        news[m][...] = new
        part(copies[m], m, me)[...] = new.astype(jnp.bfloat16)
        for direction in range(2):
            @pl.when(mirror(direction, me) < n - 1)
            def _():
                ag_copy(direction, m, me).start()

    def relay(m, direction, s):
        place = mirror(direction, me)
        t = mirror(direction, jnp.maximum(place - 1 - s, 0))

        @pl.when(place - 1 - s >= 0)
        def _():
            ag_copy(direction, m, t).wait_recv()

        @pl.when((place - 1 - s >= 0) & (place < n - 1))
        def _():
            ag_copy(direction, m, t).start()

    def norm_copies(d):
        to = lax.rem(me + d, n)
        return [pltpu.make_async_remote_copy(
            src_ref=src, dst_ref=dst.at[me], send_sem=no_s.at[i, d - 1], recv_sem=no_r.at[i, d - 1],
            device_id={"replica": to}, device_id_type=MESH)
            for i, (src, dst) in enumerate(((gnorm_in, ng), (wnorm_in, nw), (mnorm_in, nmo)))]

    def reduce_scatter(m):
        for t in range(n):
            g_copy(m, t).wait()
        for s in range(n - 1):
            rs_step(m, near, s)
            rs_step(m, 1 - near, s)

    pl.semaphore_wait(barrier, n - 1 + nm - 1)
    for m in range(k):
        reduce_scatter(m)
        if m == 0:
            for d in range(1, n):
                for c in norm_copies(d):
                    c.start()
            ng[me] = gnorm_in[...]
            nw[me] = wnorm_in[...]
            nmo[me] = mnorm_in[...]
        own_stat(m)
        total_of(m)
        if m >= 1:
            update(m - 1)
        if m >= 2:
            for s in range(n - 1):
                for direction in range(2):
                    relay(m - 2, direction, s)
    update(k - 1)
    for d in range(1, n):
        for c in norm_copies(d):
            c.wait_recv()
    width = wnorm_in.shape[1]
    mean = functools.reduce(jnp.add, [ng[t] for t in range(n)]) * rate
    for t in range(n):
        state = hold_rate * nmo[t] + mean[:, t * width:(t + 1) * width]
        new = nw[t] - learn_rate * state
        copy_norm[:, t * width:(t + 1) * width] = new.astype(jnp.bfloat16)

        @pl.when(me == t)
        def _():
            state_norm[...] = state
            new_norm[...] = new
    for m in range(max(k - 2, 0), k):
        for s in range(n - 1):
            for direction in range(2):
                relay(m, direction, s)
    for d in range(1, n):
        for c in norm_copies(d):
            c.wait_send()
    for m in range(k):
        for d in range(1, nm):
            stat_copy(m, d).wait_send()
        for direction in range(2):
            place = mirror(direction, me)
            for s in range(n):
                t = mirror(direction, n - 1 - s)

                @pl.when(n - 1 - s > place)
                def _():
                    rs_copy(direction, m, t, neighbour(direction)).wait_send()

                @pl.when((n - 1 - s <= place) & (place < n - 1))
                def _():
                    ag_copy(direction, m, t).wait_send()


def fused(n, nm, *args):
    k = 4
    grads, weights, moments = args[:k], args[k + 1:2 * k + 1], args[2 * k + 2:3 * k + 2]
    gnorm, wnorm, mnorm = args[k], args[2 * k + 1], args[3 * k + 2]
    mats = tuple(0 if g.shape[1] != w.shape[0] else 1 for g, w in zip(grads, weights))
    rows, cols = weights[0].shape
    f32, b16 = jnp.float32, jnp.bfloat16
    width = wnorm.shape[0]
    any_, vmem = pl.BlockSpec(memory_space=pl.ANY), pl.BlockSpec(memory_space=pltpu.VMEM)
    shape = jax.ShapeDtypeStruct
    out_shape = (
        [shape(g.shape[1:], b16) for g in grads] + [shape((1, n * width), b16)]
        + [shape((rows, cols), f32)] * k + [shape((1, width), f32)]
        + [shape((rows, cols), f32)] * k + [shape((1, width), f32)]
    )
    dma = pltpu.SemaphoreType.DMA
    outs = pl.pallas_call(
        functools.partial(kernel, n, nm, mats),
        out_shape=out_shape,
        in_specs=([any_] * k + [vmem]) * 3,
        out_specs=[vmem] * len(out_shape),
        scratch_shapes=[
            pltpu.VMEM((k, n, rows, cols), f32),
            pltpu.VMEM((k, rows, cols), f32),
            pltpu.VMEM((k, rows, cols), f32),
            pltpu.VMEM((2, k, n, rows + 8, cols), b16),
            pltpu.VMEM((2, k, n, rows + 8, cols), b16),
            pltpu.VMEM((k, rows, cols), f32),
            pltpu.VMEM((k, 2, cols), f32),
            pltpu.VMEM((k, nm - 1, 2, cols), f32),
            pltpu.VMEM((n, 1, n * width), f32),
            pltpu.VMEM((n, 1, width), f32),
            pltpu.VMEM((n, 1, width), f32),
            dma((k, n)), dma((k,)), dma((k,)),
            dma((2, k, n)), dma((2, k, n)), dma((2, k, n)), dma((2, k, n)),
            dma((k, nm - 1)), dma((k, nm - 1)), dma((3, n - 1)), dma((3, n - 1)),
        ],
        compiler_params=pltpu.CompilerParams(
            collective_id=0, has_side_effects=True, vmem_limit_bytes=48 * 2**20
        ),
    )(*grads, gnorm, *weights, wnorm.reshape(1, width), *moments, mnorm.reshape(1, width))
    outs = list(outs)
    for i in range(k, len(outs), k + 1):
        outs[i] = outs[i].reshape(-1)
    return tuple(outs)


def pick(n, nm, *args):
    weights = args[5:9]
    fits = all(w.shape == weights[0].shape and w.shape[0] == w.shape[1] and w.shape[0] % 128 == 0 for w in weights)
    if 1 < n <= 4 and nm > 1 and fits and args[9].shape[0] % 128 == 0:
        return fused(n, nm, *args)
    return local(*args)


def solution(mesh):
    placed = (
        P(("job", "replica"), None, "model"),
        P(("job", "replica"), None, "model"),
        P(("job", "replica"), None, "model"),
        P(("job", "replica"), "model", None),
        P(("job", "replica"), None),
        P(("job", "replica"), "model"),
        P(("job", "replica"), "model"),
        P(("job", "replica"), "model"),
        P(("job", "model"), "replica"),
        P(("job", "replica")),
        P(("job", "replica"), "model"),
        P(("job", "replica"), "model"),
        P(("job", "replica"), "model"),
        P(("job", "model"), "replica"),
        P(("job", "replica")),
    )
    return jax.shard_map(
        functools.partial(pick, mesh.shape["replica"], mesh.shape["model"]),
        mesh=mesh,
        in_specs=placed,
        out_specs=(
            P("job", "model"),
            P("job", "model"),
            P("job", "model"),
            P(("job", "model"), None),
            P("job"),
            P(("job", "replica"), "model"),
            P(("job", "replica"), "model"),
            P(("job", "replica"), "model"),
            P(("job", "model"), "replica"),
            P(("job", "replica")),
            P(("job", "replica"), "model"),
            P(("job", "replica"), "model"),
            P(("job", "replica"), "model"),
            P(("job", "model"), "replica"),
            P(("job", "replica")),
        ),
        check_vma=False,
    )
```

```python
import functools

import jax
import jax.numpy as jnp
from jax import lax
from jax.experimental import pallas as pl
from jax.experimental.pallas import tpu as pltpu
from jax.sharding import PartitionSpec as P

learn_rate = 0.5
hold_rate = 0.9


def local(
    grad_query,
    grad_key,
    grad_value,
    grad_mixed,
    grad_norm,
    weight_query,
    weight_key,
    weight_value,
    weight_mixed,
    weight_norm,
    moment_query,
    moment_key,
    moment_value,
    moment_mixed,
    moment_norm,
):
    mean_query, mean_key, mean_value, mean_mixed = (
        lax.psum_scatter(grad_query[0], "replica", scatter_dimension=0, tiled=True),
        lax.psum_scatter(grad_key[0], "replica", scatter_dimension=0, tiled=True),
        lax.psum_scatter(grad_value[0], "replica", scatter_dimension=0, tiled=True),
        lax.psum_scatter(grad_mixed[0], "replica", scatter_dimension=1, tiled=True),
    )
    whole_norm = lax.psum(grad_norm[0], "replica")
    place = lax.axis_index("replica")
    mean_norm = lax.dynamic_slice_in_dim(
        whole_norm, place * weight_norm.shape[0], weight_norm.shape[0]
    )
    mean_rate = lax.axis_size("replica") ** (-0.5)
    mean_query = mean_query * mean_rate
    mean_key = mean_key * mean_rate
    mean_value = mean_value * mean_rate
    mean_mixed = mean_mixed * mean_rate
    mean_norm = mean_norm * mean_rate
    (
        own_query,
        own_key,
        own_value,
        own_mixed,
        slope_query_norm,
        slope_key_norm,
        slope_value_norm,
        slope_mixed_norm,
    ) = lax.psum(
        (
            jnp.sum(weight_query * weight_query, axis=1, keepdims=True),
            jnp.sum(weight_key * weight_key, axis=1, keepdims=True),
            jnp.sum(weight_value * weight_value, axis=1, keepdims=True),
            jnp.sum(weight_mixed * weight_mixed, axis=0, keepdims=True),
            jnp.sum(mean_query * mean_query, axis=1, keepdims=True),
            jnp.sum(mean_key * mean_key, axis=1, keepdims=True),
            jnp.sum(mean_value * mean_value, axis=1, keepdims=True),
            jnp.sum(mean_mixed * mean_mixed, axis=0, keepdims=True),
        ),
        "model",
    )
    mean_query = mean_query * (jnp.sqrt(own_query) * lax.rsqrt(slope_query_norm + 1e-06))
    mean_key = mean_key * (jnp.sqrt(own_key) * lax.rsqrt(slope_key_norm + 1e-06))
    mean_value = mean_value * (jnp.sqrt(own_value) * lax.rsqrt(slope_value_norm + 1e-06))
    mean_mixed = mean_mixed * (jnp.sqrt(own_mixed) * lax.rsqrt(slope_mixed_norm + 1e-06))
    state_new_query = hold_rate * moment_query + mean_query
    new_query = weight_query - learn_rate * state_new_query
    state_new_key = hold_rate * moment_key + mean_key
    new_key = weight_key - learn_rate * state_new_key
    state_new_value = hold_rate * moment_value + mean_value
    new_value = weight_value - learn_rate * state_new_value
    state_new_mixed = hold_rate * moment_mixed + mean_mixed
    new_mixed = weight_mixed - learn_rate * state_new_mixed
    state_new_norm = hold_rate * moment_norm + mean_norm
    new_norm = weight_norm - learn_rate * state_new_norm
    copy_query, copy_key, copy_value, copy_mixed, copy_norm = (
        lax.all_gather(new_query.astype(jnp.bfloat16), "replica", axis=0, tiled=True),
        lax.all_gather(new_key.astype(jnp.bfloat16), "replica", axis=0, tiled=True),
        lax.all_gather(new_value.astype(jnp.bfloat16), "replica", axis=0, tiled=True),
        lax.all_gather(new_mixed.astype(jnp.bfloat16), "replica", axis=1, tiled=True),
        lax.all_gather(new_norm.astype(jnp.bfloat16), "replica", axis=0, tiled=True),
    )
    return (
        copy_query,
        copy_key,
        copy_value,
        copy_mixed,
        copy_norm,
        new_query,
        new_key,
        new_value,
        new_mixed,
        new_norm,
        state_new_query,
        state_new_key,
        state_new_value,
        state_new_mixed,
        state_new_norm,
    )


MESH = pl.DeviceIdType.MESH
EPS = 1e-06
SPAN = 228.0
FLOOR = 2.0 ** (-125 / 32)


def encode(x, scale):
    b = jnp.abs(x) * ((SPAN * FLOOR) / scale) + FLOOR
    for _ in range(5):
        b = b * b
    return jnp.where(x < 0.0, -b, b).astype(jnp.bfloat16)


def decode(y, scale):
    y = y.astype(jnp.float32)
    r = jnp.abs(y)
    for _ in range(4):
        r = lax.rsqrt(r)
    u = (r * lax.rsqrt(r) - FLOOR) * (scale * (1.0 / (SPAN * FLOOR)))
    return jnp.where(y < 0.0, -u, u)


def kernel(n, nm, mats, *refs):
    k = len(mats)
    refs = list(refs)

    def take(count):
        out = refs[:count]
        del refs[:count]
        return out

    grads, (gnorm_in,) = take(k), take(1)
    weights, (wnorm_in,) = take(k), take(1)
    moments, (mnorm_in,) = take(k), take(1)
    copies, (copy_norm,) = take(k), take(1)
    news, (new_norm,) = take(k), take(1)
    states, (state_norm,) = take(k), take(1)
    G, W, M, enc, got, total, stat, statg, ng, nw, nmo = take(11)
    gsem, wsem, msem, rs_s, rs_r, ag_s, ag_r, st_s, st_r, no_s, no_r = take(11)

    rows, cols = W.shape[1], W.shape[2]
    block = 64
    me = lax.axis_index("replica")
    mm = lax.axis_index("model")
    rate = n ** (-0.5)

    def part(ref, m, t):
        if mats[m] == 0:
            return ref.at[pl.ds(pl.multiple_of(t * rows, rows), rows), :]
        return ref.at[:, pl.ds(pl.multiple_of(t * cols, cols), cols)]

    def g_copy(m, t):
        return pltpu.make_async_copy(part(grads[m].at[0], m, t), G.at[m, t], gsem.at[m, t])

    def w_copy(m):
        return pltpu.make_async_copy(weights[m], W.at[m], wsem.at[m])

    def m_copy(m):
        return pltpu.make_async_copy(moments[m], M.at[m], msem.at[m])

    barrier = pltpu.get_barrier_semaphore()
    for d in range(1, n):
        pl.semaphore_signal(barrier, 1, device_id={"replica": lax.rem(me + d, n)}, device_id_type=MESH)
    for d in range(1, nm):
        pl.semaphore_signal(barrier, 1, device_id={"model": lax.rem(mm + d, nm)}, device_id_type=MESH)
    for m in range(k):
        for t in range(n):
            g_copy(m, t).start()
        w_copy(m).start()
        m_copy(m).start()

    near = jnp.where(2 * me < n, 0, 1)

    def mirror(direction, i):
        return jnp.where(direction == 0, i, n - 1 - i)

    def rs_copy(direction, m, t, to):
        return pltpu.make_async_remote_copy(
            src_ref=enc.at[direction, m, t], dst_ref=got.at[direction, m, t],
            send_sem=rs_s.at[direction, m, t], recv_sem=rs_r.at[direction, m, t],
            device_id={"replica": to}, device_id_type=MESH)

    def neighbour(direction):
        return jnp.clip(jnp.where(direction == 0, me + 1, me - 1), 0, n - 1)

    def blocks(body):
        @pl.loop(0, rows // block)
        def _(i):
            body(pl.ds(pl.multiple_of(i * block, block), block))

    def scale_of(direction, m, t):
        return got[direction, m, t, rows:rows + 8, :].astype(jnp.float32)[0:1]

    def rs_step(m, direction, s):
        place = mirror(direction, me)
        t = mirror(direction, n - 1 - s)

        @pl.when((n - 1 - s > place) & (place > 0))
        def _():
            rs_copy(direction, m, t, neighbour(direction)).wait_recv()
            scale = scale_of(direction, m, t)

            def body(r):
                G[m, t, r, :] = G[m, t, r, :] + decode(got[direction, m, t, r, :], scale)
            blocks(body)

        @pl.when(n - 1 - s > place)
        def _():
            def largest(i, top):
                x = jnp.abs(G[m, t, pl.ds(pl.multiple_of(i * block, block), block), :])
                return jnp.maximum(top, jnp.max(x.reshape(block // 8, 8, cols), axis=0))

            top = lax.fori_loop(0, rows // block, largest, jnp.zeros((8, cols), jnp.float32))
            top = jnp.max(top, axis=0, keepdims=True) * 1.0079 + 1e-30
            top = jnp.broadcast_to(top, (8, cols)).astype(jnp.bfloat16)
            enc[direction, m, t, rows:rows + 8, :] = top
            scale = top.astype(jnp.float32)[0:1]

            def body(r):
                enc[direction, m, t, r, :] = encode(G[m, t, r, :], scale)
            blocks(body)
            rs_copy(direction, m, t, neighbour(direction)).start()

    def stat_copy(m, d):
        peer = lax.rem(mm + d, nm)
        return pltpu.make_async_remote_copy(
            src_ref=stat.at[m], dst_ref=statg.at[m, d - 1], send_sem=st_s.at[m, d - 1], recv_sem=st_r.at[m, d - 1],
            device_id={"model": peer}, device_id_type=MESH)

    def squares(x, dim):
        x = x * x
        if dim == 1:
            return jnp.sum(x, axis=0, keepdims=True)
        half = functools.reduce(jnp.add, [x[:, c:c + 128] for c in range(0, cols, 128)])
        return jnp.sum(half.T, axis=0, keepdims=True)

    def own_stat(m):
        w_copy(m).wait()
        stat[m, 0:1, :] = squares(W[m], mats[m])

    def total_of(m):
        for direction in range(2):
            @pl.when(mirror(direction, me) > 0)
            def _():
                rs_copy(direction, m, me, neighbour(direction)).wait_recv()

        def add(*directions):
            scales = {d: scale_of(d, m, me) for d in directions}

            def body(r):
                u = functools.reduce(jnp.add, [decode(got[d, m, me, r, :], scales[d]) for d in directions])
                total[m, r, :] = (G[m, me, r, :] + u) * rate
            blocks(body)

        pl.when(me == 0)(lambda: add(1))
        pl.when(me == n - 1)(lambda: add(0))
        pl.when((me > 0) & (me < n - 1))(lambda: add(0, 1))
        stat[m, 1:2, :] = squares(total[m], mats[m])
        for d in range(1, nm):
            stat_copy(m, d).start()

    def ag_copy(direction, m, t):
        piece = part(copies[m], m, t)
        return pltpu.make_async_remote_copy(
            src_ref=piece, dst_ref=piece, send_sem=ag_s.at[direction, m, t], recv_sem=ag_r.at[direction, m, t],
            device_id={"replica": neighbour(direction)}, device_id_type=MESH)

    def update(m):
        for d in range(1, nm):
            stat_copy(m, d).wait_recv()
        sums = stat[m]
        for d in range(nm - 1):
            sums = sums + statg[m, d]
        ratio = jnp.sqrt(sums[0:1]) * lax.rsqrt(sums[1:2] + EPS)
        if mats[m] == 0:
            turned = jnp.broadcast_to(ratio, (128, rows)).T
            ratio = jnp.concatenate([turned] * (cols // 128), axis=1)
        m_copy(m).wait()
        state = hold_rate * M[m] + total[m] * ratio
        new = W[m] - learn_rate * state
        states[m][...] = state
        news[m][...] = new
        part(copies[m], m, me)[...] = new.astype(jnp.bfloat16)
        for direction in range(2):
            @pl.when(mirror(direction, me) < n - 1)
            def _():
                ag_copy(direction, m, me).start()

    def relay(m, direction, s):
        place = mirror(direction, me)
        t = mirror(direction, jnp.maximum(place - 1 - s, 0))

        @pl.when(place - 1 - s >= 0)
        def _():
            ag_copy(direction, m, t).wait_recv()

        @pl.when((place - 1 - s >= 0) & (place < n - 1))
        def _():
            ag_copy(direction, m, t).start()

    def norm_copies(d):
        to = lax.rem(me + d, n)
        return [pltpu.make_async_remote_copy(
            src_ref=src, dst_ref=dst.at[me], send_sem=no_s.at[i, d - 1], recv_sem=no_r.at[i, d - 1],
            device_id={"replica": to}, device_id_type=MESH)
            for i, (src, dst) in enumerate(((gnorm_in, ng), (wnorm_in, nw), (mnorm_in, nmo)))]

    def reduce_scatter(m):
        for t in range(n):
            g_copy(m, t).wait()
        for s in range(n - 1):
            rs_step(m, near, s)
            rs_step(m, 1 - near, s)

    pl.semaphore_wait(barrier, n - 1 + nm - 1)
    def relays(m):
        for s in range(n - 1):
            for direction in range(2):
                relay(m, direction, s)

    for i in range(k + 3):
        if i < k:
            reduce_scatter(i)
        if i == 0:
            for d in range(1, n):
                for c in norm_copies(d):
                    c.start()
            ng[me] = gnorm_in[...]
            nw[me] = wnorm_in[...]
            nmo[me] = mnorm_in[...]
        if i < k:
            own_stat(i)
        if 0 <= i - 2 < k:
            update(i - 2)
        if 0 <= i - 1 < k:
            total_of(i - 1)
        if 0 <= i - 3 < k - 2:
            relays(i - 3)
    for d in range(1, n):
        for c in norm_copies(d):
            c.wait_recv()
    width = wnorm_in.shape[1]
    mean = functools.reduce(jnp.add, [ng[t] for t in range(n)]) * rate
    for t in range(n):
        state = hold_rate * nmo[t] + mean[:, t * width:(t + 1) * width]
        new = nw[t] - learn_rate * state
        copy_norm[:, t * width:(t + 1) * width] = new.astype(jnp.bfloat16)

        @pl.when(me == t)
        def _():
            state_norm[...] = state
            new_norm[...] = new
    for m in range(k - 2, k):
        relays(m)
    for d in range(1, n):
        for c in norm_copies(d):
            c.wait_send()
    for m in range(k):
        for d in range(1, nm):
            stat_copy(m, d).wait_send()
        for direction in range(2):
            place = mirror(direction, me)
            for s in range(n):
                t = mirror(direction, n - 1 - s)

                @pl.when(n - 1 - s > place)
                def _():
                    rs_copy(direction, m, t, neighbour(direction)).wait_send()

                @pl.when((n - 1 - s <= place) & (place < n - 1))
                def _():
                    ag_copy(direction, m, t).wait_send()


def fused(n, nm, *args):
    k = 4
    grads, weights, moments = args[:k], args[k + 1:2 * k + 1], args[2 * k + 2:3 * k + 2]
    gnorm, wnorm, mnorm = args[k], args[2 * k + 1], args[3 * k + 2]
    mats = tuple(0 if g.shape[1] != w.shape[0] else 1 for g, w in zip(grads, weights))
    rows, cols = weights[0].shape
    f32, b16 = jnp.float32, jnp.bfloat16
    width = wnorm.shape[0]
    any_, vmem = pl.BlockSpec(memory_space=pltpu.HBM), pl.BlockSpec(memory_space=pltpu.VMEM)
    shape = jax.ShapeDtypeStruct
    out_shape = (
        [shape(g.shape[1:], b16) for g in grads] + [shape((1, n * width), b16)]
        + [shape((rows, cols), f32)] * k + [shape((1, width), f32)]
        + [shape((rows, cols), f32)] * k + [shape((1, width), f32)]
    )
    dma = pltpu.SemaphoreType.DMA
    outs = pl.pallas_call(
        functools.partial(kernel, n, nm, mats),
        out_shape=out_shape,
        in_specs=([any_] * k + [vmem]) * 3,
        out_specs=[vmem] * len(out_shape),
        scratch_shapes=[
            pltpu.VMEM((k, n, rows, cols), f32),
            pltpu.VMEM((k, rows, cols), f32),
            pltpu.VMEM((k, rows, cols), f32),
            pltpu.VMEM((2, k, n, rows + 8, cols), b16),
            pltpu.VMEM((2, k, n, rows + 8, cols), b16),
            pltpu.VMEM((k, rows, cols), f32),
            pltpu.VMEM((k, 2, cols), f32),
            pltpu.VMEM((k, nm - 1, 2, cols), f32),
            pltpu.VMEM((n, 1, n * width), f32),
            pltpu.VMEM((n, 1, width), f32),
            pltpu.VMEM((n, 1, width), f32),
            dma((k, n)), dma((k,)), dma((k,)),
            dma((2, k, n)), dma((2, k, n)), dma((2, k, n)), dma((2, k, n)),
            dma((k, nm - 1)), dma((k, nm - 1)), dma((3, n - 1)), dma((3, n - 1)),
        ],
        compiler_params=pltpu.CompilerParams(
            collective_id=0, has_side_effects=True, vmem_limit_bytes=48 * 2**20
        ),
    )(*grads, gnorm, *weights, wnorm.reshape(1, width), *moments, mnorm.reshape(1, width))
    outs = list(outs)
    for i in range(k, len(outs), k + 1):
        outs[i] = outs[i].reshape(-1)
    return tuple(outs)


def pick(n, nm, *args):
    weights = args[5:9]
    fits = all(w.shape == weights[0].shape and w.shape[0] == w.shape[1] and w.shape[0] % 128 == 0 for w in weights)
    if 1 < n <= 4 and nm > 1 and fits and args[9].shape[0] % 128 == 0:
        return fused(n, nm, *args)
    return local(*args)


def solution(mesh):
    placed = (
        P(("job", "replica"), None, "model"),
        P(("job", "replica"), None, "model"),
        P(("job", "replica"), None, "model"),
        P(("job", "replica"), "model", None),
        P(("job", "replica"), None),
        P(("job", "replica"), "model"),
        P(("job", "replica"), "model"),
        P(("job", "replica"), "model"),
        P(("job", "model"), "replica"),
        P(("job", "replica")),
        P(("job", "replica"), "model"),
        P(("job", "replica"), "model"),
        P(("job", "replica"), "model"),
        P(("job", "model"), "replica"),
        P(("job", "replica")),
    )
    return jax.shard_map(
        functools.partial(pick, mesh.shape["replica"], mesh.shape["model"]),
        mesh=mesh,
        in_specs=placed,
        out_specs=(
            P("job", "model"),
            P("job", "model"),
            P("job", "model"),
            P(("job", "model"), None),
            P("job"),
            P(("job", "replica"), "model"),
            P(("job", "replica"), "model"),
            P(("job", "replica"), "model"),
            P(("job", "model"), "replica"),
            P(("job", "replica")),
            P(("job", "replica"), "model"),
            P(("job", "replica"), "model"),
            P(("job", "replica"), "model"),
            P(("job", "model"), "replica"),
            P(("job", "replica")),
        ),
        check_vma=False,
    )
```
